32 devices in a mesh: seq: 4 (over x, core), vocab: 8 (over z, y).
Axes of the slice: x: 2, y: 2, z: 4, core: 2. Of those that a mesh axis runs over, the one named last changes fastest.
Arguments:
- hidden: bfloat16 [512, 4608], P('seq', 'vocab'), may hold values from -6 to 6
- norm_gain: float32 [4608], replicated, may hold values from -1.5 to 1.5
- unembed: bfloat16 [256000, 4608], P(('seq', 'vocab')), may hold values from -0.375 to 0.375
- targets: int32 [512], P('seq'), may hold values from 0 to 255999
Outputs:
- log_prob: float32 [512], P('seq')
- entropy: float32 [512], P('seq')
The draws below stay inside these ranges and needn't reach their ends.
All inputs are finite; a program needn't handle non-finite values.
Results may differ from the reference program's by a relative error of at most 0.0012.
Values may be sent and summed in bfloat16 or wider, within the bound.
A program may use at most 128 MiB of HBM per device.

```python
import jax
import jax.numpy as jnp
from jax import lax

D = 4608
VOCAB = 256000
TOKENS = 512


def touch_ends(values, stream_key, low, top_value):
    longest = values.shape.index(max(values.shape))
    spots = []
    for shift in (0, 1):
        where = [jax.random.randint(jax.random.fold_in(stream_key, axis), (), 0, length) for axis, length in enumerate(values.shape)]
        where[longest] = (where[longest] + shift) % values.shape[longest]
        spots.append(tuple(where))
    return values.at[spots[0]].set(low).at[spots[1]].set(top_value)


def block_levels(key, extent, split, least, largest):
    level = 1.0
    for dim, blocks in split:
        heights = jax.random.uniform(jax.random.fold_in(jax.random.fold_in(key, 6), dim), (blocks,), jnp.float32, least / len(split), largest / len(split))
        level = level * jnp.repeat(jnp.exp(heights), extent[dim] // blocks).reshape((-1,) + (1,) * (len(extent) - 1 - dim))
    return level


def centred(rng, dims, spread, reach, pieces=(), kind=jnp.bfloat16):
    result = spread * jax.random.normal(rng, dims, jnp.float32)
    if pieces:
        result = result * block_levels(rng, dims, pieces, -0.22, 0.18)
    return jnp.clip(result, -reach, reach).astype(kind)


def setup_inputs(seed: int = 0) -> dict:
    splits = jax.random.split(jax.random.key(seed), 5)
    return {
        "hidden": centred(splits[0], (TOKENS, D), 1.0, 6.0, ((0, 4), (1, 8))),
        "norm_gain": centred(splits[1], (D,), 0.3, 1.5, (), jnp.float32),
        "unembed": centred(splits[2], (VOCAB, D), (D // 16) ** -0.5, 0.375, ((0, 32),)),
        "targets": touch_ends(jax.random.randint(splits[3], (TOKENS,), 0, VOCAB), jax.random.fold_in(splits[3], 1), 0, VOCAB - 1).astype(jnp.int32),
    }


softcap = 30.0
epsilon = 1e-06

def normalize(hidden, norm_gain):
    values = hidden.astype(jnp.float32)
    scale = lax.rsqrt(lax.optimization_barrier(jnp.mean(values * values, axis=1, keepdims=True)) + epsilon)
    return (values * scale * (1.0 + norm_gain.astype(jnp.float32))).astype(jnp.bfloat16)

def reference(hidden, norm_gain, unembed, targets):
    normed = normalize(hidden, norm_gain)
    blocks = unembed.reshape(32, VOCAB // 32, D)

    def block_sums(block):
        logits = lax.dot_general(normed, block, (((1,), (1,)), ((), ())), preferred_element_type=jnp.float32)
        capped = softcap * jnp.tanh(logits / softcap)
        weights = jnp.exp(capped - softcap)
        return (lax.optimization_barrier(jnp.sum(weights, axis=1)), lax.optimization_barrier(jnp.sum(weights * capped, axis=1)))
    sums, moments = lax.map(block_sums, blocks)
    total = lax.optimization_barrier(jnp.sum(sums, axis=0))
    moment = lax.optimization_barrier(jnp.sum(moments, axis=0))
    picked = unembed[targets.astype(jnp.int32)].astype(jnp.float32)
    target_logit = lax.optimization_barrier(jnp.sum(normed.astype(jnp.float32) * picked, axis=1))
    chosen = softcap * jnp.tanh(target_logit / softcap)
    log_norm = softcap + jnp.log(total)
    return (chosen - log_norm, log_norm - moment / total)
```

```python
import functools

import jax
import jax.numpy as jnp
from jax import lax
from jax.experimental import pallas as pl
from jax.experimental.pallas import tpu as pltpu
from jax.sharding import PartitionSpec as P

softcap = 30.0
epsilon = 1e-06
CORES = 2
QUARTERS = 4
MESH = pl.DeviceIdType.MESH
ORDERS = (("x", "y", "z"), ("y", "x", "z"), ("z", "x", "y"), ("z", "y", "x"))


def gather_kernel(sizes, hidden_ref, gain_ref, targets_ref, normed_ref, all_targets_ref,
                  held, load_sem, send_sem, recv_sem, pair_send, pair_recv, id_send, id_recv):
    X, Y, Z = sizes["x"], sizes["y"], sizes["z"]
    seq, vocab = lax.axis_index("seq"), lax.axis_index("vocab")
    core = lax.rem(seq, CORES)
    me = {"x": seq // CORES, "y": lax.rem(vocab, Y), "z": vocab // Y}
    rows, part = held.shape[5], held.shape[6]

    def device(**moved):
        at = {**me, **moved}
        return {"seq": at["x"] * CORES + at.get("core", core), "vocab": at["z"] * Y + at["y"]}

    loads = [
        pltpu.make_async_copy(
            hidden_ref.at[pl.ds(q * rows, rows)],
            held.at[core, q, me["z"], me["y"], me["x"]],
            load_sem.at[q],
        )
        for q in range(QUARTERS)
    ]
    for load in loads:
        load.start()

    seqs = X * CORES
    greeted = [{"seq": lax.rem(seq + k, seqs), "vocab": vocab} for k in range(1, seqs)]
    for d in ("y", "z"):
        n = sizes[d]
        for k in sorted({1, n - 1}) if n > 1 else ():
            greeted.append(device(**{d: lax.rem(me[d] + k, n)}))
    barrier = pltpu.get_barrier_semaphore()
    for other in greeted:
        pl.semaphore_signal(barrier, inc=1, device_id=other, device_id_type=MESH)
    all_targets_ref[seq] = targets_ref[...]
    for load in loads:
        load.wait()
    pl.semaphore_wait(barrier, len(greeted))

    sends = []

    def targets_copy(k, to, slot):
        return pltpu.make_async_remote_copy(
            src_ref=targets_ref, dst_ref=all_targets_ref.at[slot],
            send_sem=id_send.at[k - 1], recv_sem=id_recv.at[k - 1],
            device_id={"seq": to, "vocab": vocab}, device_id_type=MESH,
        )

    def quarter(q):
        done = set()
        for axis, d in enumerate(ORDERS[q]):
            n = sizes[d]
            ahead = n // 2 if q % 2 == 0 else (n - 1) // 2
            behind = n - 1 - ahead

            def region(i):
                index = tuple(
                    i if e == d else (pl.ds(0, sizes[e]) if e in done else me[e]) for e in ("z", "y", "x")
                )
                return held.at[(core, q) + index]

            def copy(step, way):
                i = lax.rem(me[d] + (n - step + 1 if way == 0 else step - 1), n)
                sem = (q, axis, way, step - 1)
                return pltpu.make_async_remote_copy(
                    src_ref=region(i), dst_ref=region(i),
                    send_sem=send_sem.at[sem], recv_sem=recv_sem.at[sem],
                    device_id=device(**{d: lax.rem(me[d] + (1 if way == 0 else n - 1), n)}),
                    device_id_type=MESH,
                )

            for step in range(1, max(ahead, behind) + 1):
                going = [copy(step, w) for w, last in ((0, ahead), (1, behind)) if step <= last]
                for c in going:
                    c.start()
                sends.extend(going)
                yield
                for c in going:
                    c.wait_recv()
            done.add(d)
        pair = pltpu.make_async_remote_copy(
            src_ref=held.at[core, q], dst_ref=held.at[core, q],
            send_sem=pair_send.at[q], recv_sem=pair_recv.at[q],
            device_id=device(core=1 - core), device_id_type=MESH,
        )
        pair.start()
        sends.append(pair)
        pairs[q] = pair

    pairs = {}
    running = [quarter(q) for q in range(QUARTERS)]
    first = True
    while running:
        running = [g for g in running if next(g, "end") is None]
        if first:
            ids = [targets_copy(k, lax.rem(seq + k, seqs), seq) for k in range(1, seqs)]
            for c in ids:
                c.start()
            first = False
    for c in ids:
        c.wait()

    width = Z * Y * part
    for q in range(QUARTERS):
        pairs[q].wait_recv()

        def block(i, _, q=q):
            c, x = lax.rem(i, CORES), i // CORES
            squares = jnp.zeros((rows, 1), jnp.float32)
            for v in range(Z * Y):
                values = held[c, q, v // Y, v % Y, x].astype(jnp.float32)
                squares += jnp.sum(values * values, axis=1, keepdims=True)
            scale = lax.rsqrt(squares / width + epsilon)
            start = pl.multiple_of((x * CORES + c) * (rows * QUARTERS) + q * rows, rows)
            for v in range(Z * Y):
                values = held[c, q, v // Y, v % Y, x].astype(jnp.float32)
                normed_ref[pl.ds(start, rows), v * part:(v + 1) * part] = (
                    values * scale * (1.0 + gain_ref[v])
                ).astype(jnp.bfloat16)
            return 0

        lax.fori_loop(0, X * CORES, block, 0)
    for c in sends:
        c.wait_send()


def exchange_kernel(seqs, vocabs, stats_ref, log_prob_ref, entropy_ref, arrived, send_sem, recv_sem):
    count = seqs * vocabs
    seq, vocab = lax.axis_index("seq"), lax.axis_index("vocab")
    me = seq * vocabs + vocab

    def place(k):
        other = lax.rem(me + k, count)
        return other, {"seq": other // vocabs, "vocab": lax.rem(other, vocabs)}

    barrier = pltpu.get_barrier_semaphore()

    def greet(k, _):
        pl.semaphore_signal(barrier, inc=1, device_id=place(k)[1], device_id_type=MESH)
        return 0

    lax.fori_loop(1, count, greet, 0)
    arrived[me] = stats_ref[seq]
    pl.semaphore_wait(barrier, count - 1)

    def copy(k, slot):
        other, where = place(k)
        return pltpu.make_async_remote_copy(
            src_ref=stats_ref.at[other // vocabs], dst_ref=arrived.at[slot],
            send_sem=send_sem.at[k], recv_sem=recv_sem.at[slot],
            device_id=where, device_id_type=MESH,
        )

    def send(k, _):
        copy(k, me).start()
        return 0

    def sent(k, _):
        copy(k, me).wait_send()
        return 0

    def receive(k, _):
        copy(k, place(k)[0]).wait_recv()
        return 0

    lax.fori_loop(1, count, send, 0)
    lax.fori_loop(1, count, receive, 0)
    sums = arrived[0]
    for i in range(1, count):
        sums = sums + arrived[i]
    total, moment, chosen = sums[0:1], sums[1:2], sums[2:3]
    log_norm = softcap + jnp.log(total)
    log_prob_ref[...] = chosen - log_norm
    entropy_ref[...] = log_norm - moment / total
    lax.fori_loop(1, count, sent, 0)


def token_stats(logits, target_rows, first):
    capped = softcap * jnp.tanh(logits / softcap)
    weights = jnp.exp(capped - softcap)
    columns = first + lax.broadcasted_iota(jnp.int32, logits.shape, 1)
    chosen = jnp.where(columns == target_rows[:, None], capped, 0.0)
    return jnp.stack(
        [jnp.sum(weights, axis=1), jnp.sum(weights * capped, axis=1), jnp.sum(chosen, axis=1)]
    )


def on_device(seqs, vocabs, hidden, norm_gain, unembed, targets):
    vocab_rows, width = unembed.shape
    own, part = hidden.shape
    first = lax.axis_index(("seq", "vocab")) * vocab_rows
    Y = 2 ** ((vocabs.bit_length() - 1) // 2)
    sizes = {"x": seqs // CORES, "y": Y, "z": vocabs // Y}
    steps = max(max(n // 2 for n in sizes.values()), 1)
    vmem = pl.BlockSpec(memory_space=pltpu.VMEM)
    normed, all_targets = pl.pallas_call(
        functools.partial(gather_kernel, sizes),
        out_shape=(
            jax.ShapeDtypeStruct((seqs * own, width), jnp.bfloat16),
            jax.ShapeDtypeStruct((seqs, 1, own), jnp.int32),
        ),
        in_specs=[pl.BlockSpec(memory_space=pltpu.HBM), vmem, vmem],
        out_specs=(vmem, vmem),
        scratch_shapes=[
            pltpu.VMEM((CORES, QUARTERS, sizes["z"], Y, sizes["x"], own // QUARTERS, part), jnp.bfloat16),
            pltpu.SemaphoreType.DMA((QUARTERS,)),
            pltpu.SemaphoreType.DMA((QUARTERS, 3, 2, steps)),
            pltpu.SemaphoreType.DMA((QUARTERS, 3, 2, steps)),
            pltpu.SemaphoreType.DMA((QUARTERS,)),
            pltpu.SemaphoreType.DMA((QUARTERS,)),
            pltpu.SemaphoreType.DMA((seqs - 1,)),
            pltpu.SemaphoreType.DMA((seqs - 1,)),
        ],
        compiler_params=pltpu.CompilerParams(collective_id=0, has_side_effects=True),
        name="gather_norm",
    )(hidden, norm_gain.reshape(vocabs, 1, part), targets.reshape(1, own))
    logits = lax.dot_general(
        normed, unembed, (((1,), (1,)), ((), ())), preferred_element_type=jnp.float32
    )
    stats = token_stats(logits, all_targets.reshape(seqs * own), first)
    stats = jnp.transpose(stats.reshape(3, seqs, own), (1, 0, 2))
    log_prob, entropy = pl.pallas_call(
        functools.partial(exchange_kernel, seqs, vocabs),
        out_shape=(jax.ShapeDtypeStruct((1, own), jnp.float32),) * 2,
        in_specs=[vmem],
        out_specs=(vmem, vmem),
        scratch_shapes=[
            pltpu.VMEM((seqs * vocabs, 3, own), jnp.float32),
            pltpu.SemaphoreType.DMA((seqs * vocabs,)),
            pltpu.SemaphoreType.DMA((seqs * vocabs,)),
        ],
        compiler_params=pltpu.CompilerParams(collective_id=1, has_side_effects=True),
        name="exchange",
    )(stats)
    return log_prob.reshape(own), entropy.reshape(own)


def solution(mesh):
    return jax.shard_map(
        functools.partial(on_device, mesh.shape["seq"], mesh.shape["vocab"]),
        mesh=mesh,
        in_specs=(P("seq", "vocab"), P(), P(("seq", "vocab"), None), P("seq")),
        out_specs=(P("seq"), P("seq")),
        check_vma=False,
    )
```
